32 devices in a mesh: freq: 4 (over x, core), gblk: 8 (over z, y).
Axes of the slice: x: 2, y: 2, z: 4, core: 2. Of those that a mesh axis runs over, the one named last changes fastest.
Arguments:
- w_imag: bfloat16 [8, 8192, 16384], P('freq', 'gblk'), may hold values from -0.046875 to 0.046875
- w_real: bfloat16 [4, 8192, 16384], P('freq', 'gblk'), may hold values from -0.046875 to 0.046875
- pair_elements: bfloat16 [8192, 256], P('gblk'), may hold values from -0.75 to 0.75
- quad_weight: float32 [8, 128], P('freq'), may hold values from 0.1 to 1
- residue_freq: int32 [128], replicated, may hold values from 0 to 3
- owner_bands: int32 [128], replicated, may hold values from 0 to 127, each once
Outputs:
- sigma: float32 [128, 256], P(('freq', 'gblk'))
The draws below stay inside these ranges and needn't reach their ends.
Inputs may be any that keep to these rules, and one draw needn't show every extreme that they name: `owner_bands`: each band appears once.
All inputs are finite; a program needn't handle non-finite values.
Results may differ from the reference program's by a relative error of at most 0.0003.
Values may be sent and summed in bfloat16 or wider, within the bound.
A program may use at most 192 MiB of HBM per device.

```python
import math
import jax
import jax.numpy as jnp
from jax import lax

NG = 8192
NB = 128
NFI = 8
NFR = 4


def set_ends(result, stream_key, low, top_value):
    longest = result.shape.index(max(result.shape))
    spots = []
    for shift in (0, 1):
        where = [jax.random.randint(jax.random.fold_in(stream_key, axis), (), 0, length) for axis, length in enumerate(result.shape)]
        where[longest] = (where[longest] + shift) % result.shape[longest]
        spots.append(tuple(where))
    return result.at[spots[0]].set(low).at[spots[1]].set(top_value)


def strengthened(values, stream_key, source, target, blocks, factor):
    owner, partner = [(jnp.arange(values.shape[position]) // (values.shape[position] // blocks)).reshape([-1 if axis == position else 1 for axis in range(values.ndim)]) for position in (source, target)]
    chosen = jax.random.permutation(stream_key, blocks)[partner]
    strong = (owner == chosen) | (owner == (partner + blocks // 2) % blocks)
    return jnp.where(strong, factor * values, values)


def block_scale(stream_key, extent, shards, smallest, largest):
    def one(dim, parts):
        steps = jax.random.uniform(jax.random.fold_in(jax.random.fold_in(stream_key, 6), dim), (parts,), jnp.float32, smallest / len(shards), largest / len(shards))
        return jnp.repeat(jnp.exp(steps), extent[dim] // parts).reshape((-1,) + (1,) * (len(extent) - dim - 1))

    factor_of = one(*shards[0])
    for cut in shards[1:]:
        factor_of = factor_of * one(*cut)
    return factor_of


def scatter_about(rng, dims, spread, reach, split=(), held_as=jnp.bfloat16):
    loudness = block_scale(rng, dims, split, -0.22, 0.18) if split else 1.0
    entries = jax.random.normal(rng, dims, jnp.float32) * spread * loudness
    return jnp.minimum(jnp.maximum(entries, -reach), reach).astype(held_as)


def noise_with(rng, dims, scale, limit, cuts, heavy, kind=jnp.bfloat16):
    drawn = scale * jax.random.normal(rng, dims, jnp.float32)
    if cuts:
        drawn = drawn * block_scale(rng, dims, cuts, -0.22, 0.18)
    return jnp.clip(strengthened(drawn, jax.random.fold_in(rng, 3), *heavy), -limit, limit).astype(kind)


def setup_inputs(seed: int = 0) -> dict:
    keys = jax.random.split(jax.random.key(seed), 7)
    w_imag = scatter_about(keys[0], (NFI, NG, 2 * NG), (2 * NG) ** -0.5, 0.046875, ((0, 4), (1, 8)))
    w_real = scatter_about(keys[1], (NFR, NG, 2 * NG), (2 * NG) ** -0.5, 0.046875, ((0, 4), (1, 8)))
    pair_elements = noise_with(keys[2], (NG, 2 * NB), 0.09, 0.75, ((0, 8),), (0, 1, 8, 2.0))
    quad_weight = jnp.clip(jnp.exp(math.log(1.0) - 2.3025851 * jax.random.uniform(keys[3], (NFI, NB), jnp.float32) ** block_scale(keys[3], (NFI, NB), ((0, 4),), -0.2, 0.2)), 0.1, 1.0)
    residue_freq = set_ends(jax.random.randint(keys[4], (NB,), 0, NFR), jax.random.fold_in(keys[4], 1), 0, NFR - 1).astype(jnp.int32)
    owner_bands = jax.random.permutation(keys[5], NB).astype(jnp.int32)
    return {"w_imag": w_imag, "w_real": w_real, "pair_elements": pair_elements, "quad_weight": quad_weight, "residue_freq": residue_freq, "owner_bands": owner_bands}


def reference(w_imag, w_real, pair_elements, quad_weight, residue_freq, owner_bands):
    bands = NB
    real_part = pair_elements[:, :bands]
    imag_part = pair_elements[:, bands:]
    lower_rows = jnp.concatenate([-imag_part, real_part], axis=1)
    stacked = jnp.concatenate([pair_elements, lower_rows], axis=0).astype(jnp.float32)
    block_rows = min(NG, 1024)
    wide_elems = pair_elements.astype(jnp.float32).reshape(NG // block_rows, block_rows, 2 * bands)

    def per_frequency(matrix):
        pieces = matrix.reshape(NG // block_rows, block_rows, 2 * NG)

        def per_block(packed):
            w_block, m_block = packed
            x_block = jnp.dot(w_block.astype(jnp.float32), stacked, precision=lax.Precision.HIGHEST)
            return jnp.dot(m_block.T, x_block, precision=lax.Precision.HIGHEST)

        blocks = jnp.sum(lax.map(per_block, (pieces, wide_elems)), axis=0)
        sig_re = blocks[:bands, :bands] + blocks[bands:, bands:]
        sig_im = blocks[:bands, bands:] - blocks[bands:, :bands]
        return jnp.concatenate([sig_re, sig_im], axis=1)

    s_imag = lax.map(per_frequency, w_imag)
    s_real = lax.map(per_frequency, w_real)
    residue_weight = (residue_freq[None, :] == jnp.arange(NFR, dtype=jnp.int32)[:, None]).astype(jnp.float32)
    total = jnp.sum(quad_weight[:, :, None] * s_imag, axis=0) + jnp.sum(residue_weight[:, :, None] * s_real, axis=0)
    return total[owner_bands]
```

```python
import functools

import jax
import jax.numpy as jnp
from jax import lax
from jax.experimental import pallas as pl
from jax.experimental.pallas import tpu as pltpu
from jax.sharding import PartitionSpec as P

MESH = pl.DeviceIdType.MESH
EDGE = 256
UNITS = 2
BUFFERS = 3
POP_AT = 2


def ring_position(index, n):
    z = index // 2
    return z + (index % 2) * (n - 1 - 2 * z)


def ring_index(position, n):
    low = (position < n // 2).astype(jnp.int32)
    return low * (2 * position) + (1 - low) * (2 * (n - 1 - position) + 1)


class Plan:
    def __init__(self, n, nf, rows, g_count, jobs):
        assert n % 2 == 0 and n > 2 and rows % EDGE == 0 and g_count % (UNITS * EDGE) == 0
        self.n, self.nf, self.rows, self.jobs = n, nf, rows, jobs
        self.devices = n * nf
        self.tile = UNITS * EDGE
        self.steps = g_count // self.tile
        self.per_block = rows // EDGE
        assert self.per_block == 1 or self.per_block % UNITS == 0
        self.halves = 2 if rows >= 1024 else 1
        self.piece_rows = rows // (2 * self.halves)
        self.pieces = EDGE // self.piece_rows
        self.split = (self.halves + 1) // 2
        whole = (n // 2 - 1) * self.halves
        self.plus = whole + self.split
        self.minus = whole + self.halves - self.split
        self.whole = whole
        self.events = max(self.plus, self.minus)
        if self.steps >= 2 * self.events:
            self.num, self.den, self.first = 3, 2, 4
        else:
            self.num, self.den, self.first = 1, 1, 1
        at = [self.first + (m * self.num) // self.den for m in range(self.events)]
        self.looped = sum(1 for a in at if a < self.steps)
        self.at = at
        lag = 2
        for k in range(1, n):
            need = (k * self.per_block) // UNITS
            last = max(self.at[m] for m in range(self.events) if k in self.blocks_of(m))
            lag = max(lag, last + 2 - need)
        self.lag = min(lag, self.steps - 2)

    def blocks_of(self, m):
        found = []
        if m < self.plus:
            found.append(2 * (m // self.halves) + 1)
        if m < self.minus:
            found.append(min(2 * (m // self.halves) + 2, self.n - 1))
        return found


def self_energy_kernel(
    plan,
    wi_hbm, wr_hbm, m_hbm, quad_hbm, residue_hbm, owner_hbm, out_ref,
    wbuf, gath, left, weights, uacc, ubuf, quad_ref, residue_ref, owner_ref, stage, inbox,
    w_sem, own_sem, small_sem, ring_send, ring_recv, pair_send, pair_recv, out_send, out_recv,
):
    def body(*accs):
        run(
            plan, accs[:UNITS], (accs[UNITS:2 * UNITS], accs[2 * UNITS:3 * UNITS], accs[3 * UNITS:]),
            wi_hbm, wr_hbm, m_hbm, quad_hbm, residue_hbm, owner_hbm, out_ref,
            wbuf, gath, left, weights, uacc, ubuf, quad_ref, residue_ref, owner_ref, stage, inbox,
            w_sem, own_sem, small_sem, ring_send, ring_recv, pair_send, pair_recv, out_send, out_recv)

    shape = (EDGE, EDGE)
    pl.run_scoped(body, *[pltpu.ACC(i % UNITS)(shape, jnp.float32) for i in range(4 * UNITS)])


def run(
    plan, vacc, uaccs,
    wi_hbm, wr_hbm, m_hbm, quad_hbm, residue_hbm, owner_hbm, out_ref,
    wbuf, gath, left, weights, uacc, ubuf, quad_ref, residue_ref, owner_ref, stage, inbox,
    w_sem, own_sem, small_sem, ring_send, ring_recv, pair_send, pair_recv, out_send, out_recv,
):
    n, nf, rows, jobs = plan.n, plan.nf, plan.rows, plan.jobs
    halves, piece_rows, steps, lag = plan.halves, plan.piece_rows, plan.steps, plan.lag
    per_block, devices, split = plan.per_block, plan.devices, plan.split
    f = lax.axis_index("freq")
    me = lax.axis_index("gblk")
    pos = ring_position(me, n)
    core = f % 2
    fi = wi_hbm.shape[0]
    fr = wr_hbm.shape[0]
    g_count = wi_hbm.shape[2] // 2
    bands = owner_ref.shape[1]
    mine = f * n + me
    chunks = [(part, c) for part in range(2) for c in range(rows // EDGE)]

    def slot_of(k):
        d = (k + 1) // 2
        sign = 2 * (k % 2) - 1
        return lax.rem(pos - sign * d + 2 * n, n)

    def w_source(j, part, col, width):
        cols = pl.ds(pl.multiple_of(col + part * g_count, EDGE), width)
        return wi_hbm.at[j, :, cols] if j < fi else wr_hbm.at[j - fi, :, cols]

    def start_w(t, slot, j):
        for part in range(2):
            if per_block == 1:
                for q in range(UNITS):
                    col = ring_index(slot_of(UNITS * t + q), n) * rows
                    pltpu.make_async_copy(
                        w_source(j, part, col, EDGE),
                        wbuf.at[slot, j, part, :, pl.ds(q * EDGE, EDGE)], w_sem.at[slot, j]).start()
            else:
                trips = per_block // UNITS
                col = ring_index(slot_of(t // trips), n) * rows + (t % trips) * plan.tile
                pltpu.make_async_copy(
                    w_source(j, part, col, plan.tile), wbuf.at[slot, j, part], w_sem.at[slot, j]).start()

    def wait_w(slot, j):
        pltpu.make_async_copy(wbuf.at[slot, j], wbuf.at[slot, j], w_sem.at[slot, j]).wait()

    small = [
        pltpu.make_async_copy(owner_hbm, owner_ref, small_sem.at[0]),
        pltpu.make_async_copy(quad_hbm, quad_ref, small_sem.at[1]),
        pltpu.make_async_copy(residue_hbm, residue_ref, small_sem.at[2]),
    ]
    own = [pltpu.make_async_copy(
        m_hbm.at[pl.ds(i * piece_rows, piece_rows)], gath.at[pos, i], own_sem.at[i])
        for i in range(2 * halves)]
    for c in small + own:
        c.start()
    for t in range(min(BUFFERS, steps)):
        for j in range(jobs):
            start_w(t, t, j)

    barrier = pltpu.get_barrier_semaphore()

    def greet(r, carry):
        other = lax.rem(mine + r, devices)
        pl.semaphore_signal(barrier, inc=1, device_id=(other // n, other % n), device_id_type=MESH)
        return carry

    lax.fori_loop(1, devices, greet, 0)

    for acc in list(vacc) + [a for pair in uaccs for a in pair]:
        pltpu.matmul_pop(acc)
    uacc[...] = jnp.zeros_like(uacc)

    for c in small:
        c.wait()
    onehot_t = (lax.broadcasted_iota(jnp.int32, (bands, bands), 0) == owner_ref[...]).astype(jnp.float32)
    onehot = jnp.transpose(onehot_t)
    for j in range(jobs):
        if j < fi:
            row = quad_ref[pl.ds(j, 1), :]
        else:
            row = (residue_ref[...] == f * fr + (j - fi)).astype(jnp.float32)
        column = jnp.broadcast_to(jnp.sum(onehot * row, axis=1, keepdims=True), (bands, EDGE))
        weights[j, pl.ds(0, bands), :] = column
        weights[j, pl.ds(bands, bands), :] = column
    nothing = jnp.zeros_like(onehot)
    pick = (
        jnp.concatenate([jnp.concatenate([onehot, nothing], axis=1),
                         jnp.concatenate([nothing, 0.0 - onehot], axis=1)], axis=0).astype(jnp.bfloat16),
        jnp.concatenate([jnp.concatenate([nothing, onehot], axis=1),
                         jnp.concatenate([onehot, nothing], axis=1)], axis=0).astype(jnp.bfloat16),
    )

    def m_tile(slot, sub):
        return gath[slot, pl.ds(sub * plan.pieces, plan.pieces)].reshape(EDGE, 2 * bands)

    for c in own:
        c.wait()
    for c in range(rows // EDGE):
        q = c % UNITS
        pltpu.matmul_push_rhs(m_tile(pos, c), 0, q, transpose=True)
        pltpu.matmul_acc_lhs(uaccs[0][q], pick[0], load_staged_rhs=0)
        pltpu.matmul_acc_lhs(uaccs[1][q], pick[1])
        left[0, c] = pltpu.matmul_pop(uaccs[0][q]).astype(jnp.bfloat16)
        left[1, c] = pltpu.matmul_pop(uaccs[1][q]).astype(jnp.bfloat16)

    def ring_copy(k, q, sending_slot, sign):
        to = ring_index(lax.rem(pos + sign + n, n), n)
        at = gath.at[sending_slot, core * halves + q]
        return pltpu.make_async_remote_copy(
            src_ref=at, dst_ref=at, send_sem=ring_send.at[k, q], recv_sem=ring_recv.at[k, q],
            device_id=(f, to), device_id_type=MESH)

    def pair_copy(k, q, whose):
        at = gath.at[slot_of(k), whose * halves + q]
        return pltpu.make_async_remote_copy(
            src_ref=at, dst_ref=at, send_sem=pair_send.at[k, q], recv_sem=pair_recv.at[k, q],
            device_id=(f + 1 - 2 * core, me), device_id_type=MESH)

    def start_own():
        for q in range(halves):
            ring_copy(1, q, pos, 1).start()
            ring_copy(2, q, pos, -1).start()

    def event(m):
        def plus():
            k, q = 2 * (m // halves) + 1, m % halves
            ring_copy(k, q, slot_of(k), 1).wait_recv()

            @pl.when((k + 2 < n - 1) | ((k + 2 == n - 1) & (q < split)))
            def _():
                ring_copy(k + 2, q, slot_of(k), 1).start()

            pair_copy(k, q, core).start()

        def minus():
            last = jnp.int32(m >= plan.whole) if isinstance(m, int) else (m >= plan.whole).astype(jnp.int32)
            k = (1 - last) * (2 * (m // halves) + 2) + last * (n - 1)
            q = (1 - last) * (m % halves) + last * (split + m - plan.whole)
            ring_copy(k, q, slot_of(k), -1).wait_recv()

            @pl.when((k + 2 < n - 1) | ((k == n - 2) & (q >= split)))
            def _():
                further = (k == n - 2).astype(jnp.int32)
                ring_copy((1 - further) * (k + 2) + further * (n - 1), q, slot_of(k), -1).start()

            pair_copy(k, q, core).start()

        pl.when(m < plan.plus)(plus)
        pl.when(m < plan.minus)(minus)

    def await_pair(k):
        for q in range(halves):
            pair_copy(k, q, 1 - core).wait_recv()

    def await_for(v):
        if per_block == 1:
            for q in range(UNITS):
                @pl.when((v >= 0) & (UNITS * v + q > 0))
                def _(q=q):
                    await_pair(UNITS * v + q)
        else:
            @pl.when((v > 0) & ((UNITS * v) % per_block == 0))
            def _():
                await_pair((UNITS * v) // per_block)

    def fence(t, j, final):
        slot = lax.rem(t, BUFFERS)
        if j < jobs - 1:
            wait_w(slot, j + 1)
        elif not final:
            wait_w(lax.rem(t + 1, BUFFERS), 0)

        if not final:
            @pl.when(t + BUFFERS < steps)
            def _():
                start_w(t + BUFFERS, slot, j)

        if j == jobs - 1:
            d = t - plan.first
            m = (d * plan.den + plan.num - 1) // plan.num
            pl.when((d >= 0) & ((m * plan.num) // plan.den == d) & (m < plan.events))(lambda: event(m))
            if not final:
                await_for(t + 1 - lag)

    def push_w(slot, j, part, c):
        for q in range(UNITS):
            pltpu.matmul_push_rhs(
                wbuf[slot, j, part, pl.ds(c * EDGE, EDGE), pl.ds(q * EDGE, EDGE)], 0, q)

    def push_v(v):
        for q in range(UNITS):
            i = UNITS * v + q
            pltpu.matmul_push_rhs(m_tile(slot_of(i // per_block), i % per_block), 0, q)

    def finish(t, j):
        for q in range(UNITS):
            value = weights[j] * pltpu.matmul_pop(uaccs[j % 3][q])
            if j > 0:
                value = uacc[q] + value
            if j < jobs - 1:
                uacc[q] = value
            else:
                high = value.astype(jnp.bfloat16)
                ubuf[t + 1, q, 0] = high
                ubuf[t + 1, q, 1] = (value - high.astype(jnp.float32)).astype(jnp.bfloat16)

    def v_part(v, part):
        for q in range(UNITS):
            pltpu.matmul_acc_lhs(vacc[q], ubuf[v + 1, q, part], load_staged_rhs=None if part else 0)

    def step(t, with_v, final=False):
        slot = lax.rem(t, BUFFERS)
        following = lax.rem(t + 1, BUFFERS)
        v = t - lag
        for j in range(jobs):
            for i, (part, c) in enumerate(chunks):
                end = i == len(chunks) - 1
                if end and (j < jobs - 1 or not with_v):
                    fence(t, j, final)
                lhs = left[part, c]
                for q in range(UNITS):
                    pltpu.matmul_acc_lhs(uaccs[j % 3][q], lhs, load_staged_rhs=0)
                if not end:
                    push_w(slot, j, *chunks[i + 1])
                elif j < jobs - 1:
                    push_w(slot, j + 1, *chunks[0])
                elif with_v:
                    push_v(v)
                else:
                    push_w(following, 0, *chunks[0])
                if i == min(POP_AT, len(chunks) - 1):
                    if j == 0:
                        finish(t - 1, jobs - 1)
                    else:
                        finish(t, j - 1)
        if with_v:
            fence(t, jobs - 1, final)
            v_part(v, 0)
            if not final:
                push_w(following, 0, *chunks[0])
            v_part(v, 1)

    wait_w(0, 0)
    push_w(0, 0, *chunks[0])

    def early(t, carry):
        @pl.when(t == 1)
        def _():
            pl.semaphore_wait(barrier, devices - 1)
            start_own()

        step(t, False)
        return carry

    def late(t, carry):
        step(t, True)
        return carry

    lax.fori_loop(0, lag, early, 0)
    lax.fori_loop(lag, steps - 1, late, 0)
    step(jnp.int32(steps - 1), True, final=True)
    for m in range(plan.events):
        if plan.at[m] >= steps:
            event(m)
    waited = set()
    for v in range(steps - lag, steps):
        if v == steps - 1:
            finish(steps - 1, jobs - 1)
        for q in range(UNITS):
            k, sub = (UNITS * v + q) // per_block, (UNITS * v + q) % per_block
            if sub == 0 and k > 0 and k not in waited:
                waited.add(k)
                await_pair(k)
        push_v(v)
        v_part(v, 0)
        v_part(v, 1)

    total = pltpu.matmul_pop(vacc[0]) + pltpu.matmul_pop(vacc[1])
    p = total[:bands]
    r = total[bands:]
    real = p[:, :bands] - r[:, bands:]
    imag = p[:, bands:] + r[:, :bands]
    share = out_ref.shape[0]
    for d in range(devices):
        stage[d, :, pl.ds(0, bands)] = real[d * share:(d + 1) * share]
        stage[d, :, pl.ds(bands, bands)] = imag[d * share:(d + 1) * share]

    def give(r, carry):
        other = lax.rem(mine + r, devices)
        pltpu.make_async_remote_copy(
            src_ref=stage.at[other], dst_ref=inbox.at[r - 1], send_sem=out_send, recv_sem=out_recv,
            device_id=(other // n, other % n), device_id_type=MESH).start()
        return carry

    lax.fori_loop(1, devices, give, 0)
    for q in range(halves):
        for k in range(1, n):
            forward = k % 2 == 1 if k < n - 1 else q < split
            if k <= 2:
                source = pos
            elif k < n - 1:
                source = slot_of(k - 2)
            else:
                source = slot_of(n - 3 if forward else n - 2)
            ring_copy(k, q, source, 1 if forward else -1).wait_send()
            pair_copy(k, q, core).wait_send()
    pltpu.make_async_copy(inbox, inbox, out_recv).wait()
    out_ref[...] = stage[mine] + jnp.sum(inbox[...], axis=0)
    pltpu.make_async_copy(inbox, inbox, out_send).wait()


def on_device(n, nf, w_imag, w_real, pair_elements, quad_weight, residue_freq, owner_bands):
    fi, rows, width = w_imag.shape
    fr = w_real.shape[0]
    bands = owner_bands.shape[0]
    jobs = fi + fr
    plan = Plan(n, nf, rows, width // 2, jobs)
    devices = n * nf
    share = bands // devices
    dma = pltpu.SemaphoreType.DMA
    anyspace = pl.BlockSpec(memory_space=pl.ANY)
    vmem = pl.BlockSpec(memory_space=pltpu.VMEM)
    flops = 2 * jobs * rows * width * 2 * bands
    halves = plan.halves
    return pl.pallas_call(
        functools.partial(self_energy_kernel, plan),
        out_shape=jax.ShapeDtypeStruct((share, 2 * bands), jnp.float32),
        in_specs=[anyspace] * 6,
        out_specs=vmem,
        scratch_shapes=[
            pltpu.VMEM((BUFFERS, jobs, 2, rows, plan.tile), jnp.bfloat16),
            pltpu.VMEM((n, 2 * halves, plan.piece_rows, 2 * bands), jnp.bfloat16),
            pltpu.VMEM((2, rows // EDGE, 2 * bands, EDGE), jnp.bfloat16),
            pltpu.VMEM((jobs, 2 * bands, EDGE), jnp.float32),
            pltpu.VMEM((UNITS, 2 * bands, EDGE), jnp.float32),
            pltpu.VMEM((plan.steps + 1, UNITS, 2, 2 * bands, EDGE), jnp.bfloat16),
            pltpu.VMEM((fi, bands), jnp.float32),
            pltpu.VMEM((1, bands), jnp.int32),
            pltpu.VMEM((1, bands), jnp.int32),
            pltpu.VMEM((devices, share, 2 * bands), jnp.float32),
            pltpu.VMEM((devices - 1, share, 2 * bands), jnp.float32),
            dma((BUFFERS, jobs)),
            dma((2 * halves,)),
            dma((3,)),
            dma((n, halves)),
            dma((n, halves)),
            dma((n, halves)),
            dma((n, halves)),
            dma,
            dma,
        ],
        compiler_params=pltpu.CompilerParams(
            collective_id=0, has_side_effects=True, vmem_limit_bytes=60 * 1024 * 1024),
        cost_estimate=pl.CostEstimate(
            flops=flops, bytes_accessed=jobs * rows * width * 2, transcendentals=0),
    )(w_imag, w_real, pair_elements, quad_weight,
      residue_freq.reshape(1, bands), owner_bands.reshape(1, bands))


def solution(mesh):
    placed = (
        P("freq", "gblk", None),
        P("freq", "gblk", None),
        P("gblk", None),
        P("freq", None),
        P(),
        P(),
    )
    body = functools.partial(on_device, mesh.shape["gblk"], mesh.shape["freq"])
    return jax.shard_map(
        body, mesh=mesh, in_specs=placed, out_specs=P(("freq", "gblk"), None), check_vma=False
    )
```

```python
import functools

import jax
import jax.numpy as jnp
from jax import lax
from jax.experimental import pallas as pl
from jax.experimental.pallas import tpu as pltpu
from jax.sharding import PartitionSpec as P

MESH = pl.DeviceIdType.MESH
EDGE = 256
UNITS = 2
BUFFERS = 3
POP_AT = 2
FIRST = 2


def ring_position(index, n):
    z = index // 2
    return z + (index % 2) * (n - 1 - 2 * z)


def ring_index(position, n):
    low = (position < n // 2).astype(jnp.int32)
    return low * (2 * position) + (1 - low) * (2 * (n - 1 - position) + 1)


class Plan:
    def __init__(self, n, nf, rows, g_count, jobs):
        assert n % 2 == 0 and n > 2 and nf == 4 and rows % EDGE == 0 and g_count % (UNITS * EDGE) == 0
        self.n, self.nf, self.rows, self.jobs = n, nf, rows, jobs
        self.devices = n * nf
        self.tile = UNITS * EDGE
        self.steps = g_count // self.tile
        self.per_block = rows // EDGE
        assert self.per_block == 1 or self.per_block % UNITS == 0
        self.halves = 2 if rows >= 1024 else 1
        self.piece_rows = rows // (2 * self.halves)
        self.pieces = EDGE // self.piece_rows
        self.split = (self.halves + 1) // 2
        whole = (n // 2 - 1) * self.halves
        self.plus = whole + self.split
        self.minus = whole + self.halves - self.split
        self.whole = whole
        self.events = max(self.plus, self.minus)
        self.group = -(-self.events // 7)
        self.rounds = -(-self.events // self.group)
        self.num, self.den, self.first = 3, 2, FIRST * self.steps // 16
        self.at = [self.first + ((m // self.group) * self.num) // self.den for m in range(self.events)]
        assert self.at[-1] <= self.steps - 3
        lag = 2
        for k in range(1, n):
            need = (k * self.per_block) // UNITS
            last = max(self.at[m] for m in range(self.events) if k in self.blocks_of(m))
            lag = max(lag, last + 2 - need)
        self.lag = min(lag, self.steps - 2)

    def blocks_of(self, m):
        found = []
        if m < self.plus:
            found.append(2 * (m // self.halves) + 1)
        if m < self.minus:
            found.append(min(2 * (m // self.halves) + 2, self.n - 1))
        return found


def self_energy_kernel(
    plan,
    wi_hbm, wr_hbm, m_hbm, quad_hbm, residue_hbm, owner_hbm, out_ref,
    wbuf, gath, left, weights, uacc, ubuf, quad_ref, residue_ref, owner_ref, stage, inbox,
    w_sem, own_sem, small_sem, ring_send, ring_recv, pair_send, pair_recv, out_send, out_recv, plane_sem,
):
    def body(*accs):
        run(
            plan, accs[:UNITS], (accs[UNITS:2 * UNITS], accs[2 * UNITS:3 * UNITS], accs[3 * UNITS:]),
            wi_hbm, wr_hbm, m_hbm, quad_hbm, residue_hbm, owner_hbm, out_ref,
            wbuf, gath, left, weights, uacc, ubuf, quad_ref, residue_ref, owner_ref, stage, inbox,
            w_sem, own_sem, small_sem, ring_send, ring_recv, pair_send, pair_recv, out_send, out_recv, plane_sem)

    shape = (EDGE, EDGE)
    pl.run_scoped(body, *[pltpu.ACC(i % UNITS)(shape, jnp.float32) for i in range(4 * UNITS)])


def run(
    plan, vacc, uaccs,
    wi_hbm, wr_hbm, m_hbm, quad_hbm, residue_hbm, owner_hbm, out_ref,
    wbuf, gath, left, weights, uacc, ubuf, quad_ref, residue_ref, owner_ref, stage, inbox,
    w_sem, own_sem, small_sem, ring_send, ring_recv, pair_send, pair_recv, out_send, out_recv, plane_sem,
):
    n, nf, rows, jobs = plan.n, plan.nf, plan.rows, plan.jobs
    halves, piece_rows, steps, lag = plan.halves, plan.piece_rows, plan.steps, plan.lag
    per_block, devices, split = plan.per_block, plan.devices, plan.split
    f = lax.axis_index("freq")
    me = lax.axis_index("gblk")
    pos = ring_position(me, n)
    core = f % 2
    fi = wi_hbm.shape[0]
    fr = wr_hbm.shape[0]
    g_count = wi_hbm.shape[2] // 2
    bands = owner_ref.shape[1]
    mine = f * n + me
    chunks = [(part, c) for part in range(2) for c in range(rows // EDGE)]

    def slot_of(k):
        d = (k + 1) // 2
        sign = 2 * (k % 2) - 1
        return lax.rem(pos - sign * d + 2 * n, n)

    def w_source(j, part, col, width):
        cols = pl.ds(pl.multiple_of(col + part * g_count, EDGE), width)
        return wi_hbm.at[j, :, cols] if j < fi else wr_hbm.at[j - fi, :, cols]

    def start_w(t, slot, j):
        for part in range(2):
            if per_block == 1:
                for q in range(UNITS):
                    col = ring_index(slot_of(UNITS * t + q), n) * rows
                    pltpu.make_async_copy(
                        w_source(j, part, col, EDGE),
                        wbuf.at[slot, j, part, :, pl.ds(q * EDGE, EDGE)], w_sem.at[slot, j]).start(priority=1)
            else:
                trips = per_block // UNITS
                col = ring_index(slot_of(t // trips), n) * rows + (t % trips) * plan.tile
                pltpu.make_async_copy(
                    w_source(j, part, col, plan.tile), wbuf.at[slot, j, part], w_sem.at[slot, j]).start(priority=1)

    def wait_w(slot, j):
        pltpu.make_async_copy(wbuf.at[slot, j], wbuf.at[slot, j], w_sem.at[slot, j]).wait()

    small = [
        pltpu.make_async_copy(owner_hbm, owner_ref, small_sem.at[0]),
        pltpu.make_async_copy(quad_hbm, quad_ref, small_sem.at[1]),
        pltpu.make_async_copy(residue_hbm, residue_ref, small_sem.at[2]),
    ]
    own = [pltpu.make_async_copy(
        m_hbm.at[pl.ds(i * piece_rows, piece_rows)], gath.at[pos, i], own_sem.at[i])
        for i in range(2 * halves)]
    for c in small + own:
        c.start()
    for t in range(min(BUFFERS, steps)):
        for j in range(jobs):
            start_w(t, t, j)

    barrier = pltpu.get_barrier_semaphore()

    pair = (f + 1 - 2 * core, me)
    twin = (lax.rem(f + 2, nf), me)
    near = [(f, ring_index(lax.rem(pos + 1, n), n)), (f, ring_index(lax.rem(pos + n - 1, n), n)), pair, twin]
    for other in near:
        pl.semaphore_signal(barrier, inc=1, device_id=other, device_id_type=MESH)

    for acc in list(vacc) + [a for pair in uaccs for a in pair]:
        pltpu.matmul_pop(acc)
    uacc[...] = jnp.zeros_like(uacc)

    for c in small:
        c.wait()
    onehot_t = (lax.broadcasted_iota(jnp.int32, (bands, bands), 0) == owner_ref[...]).astype(jnp.float32)
    onehot = jnp.transpose(onehot_t)
    for j in range(jobs):
        if j < fi:
            row = quad_ref[pl.ds(j, 1), :]
        else:
            row = (residue_ref[...] == f * fr + (j - fi)).astype(jnp.float32)
        column = jnp.broadcast_to(jnp.sum(onehot * row, axis=1, keepdims=True), (bands, EDGE))
        weights[j, pl.ds(0, bands), :] = column
        weights[j, pl.ds(bands, bands), :] = column
    nothing = jnp.zeros_like(onehot)
    pick = (
        jnp.concatenate([jnp.concatenate([onehot, nothing], axis=1),
                         jnp.concatenate([nothing, 0.0 - onehot], axis=1)], axis=0).astype(jnp.bfloat16),
        jnp.concatenate([jnp.concatenate([nothing, onehot], axis=1),
                         jnp.concatenate([onehot, nothing], axis=1)], axis=0).astype(jnp.bfloat16),
    )

    def m_tile(slot, sub):
        return gath[slot, pl.ds(sub * plan.pieces, plan.pieces)].reshape(EDGE, 2 * bands)

    def ring_copy(k, q, sending_slot, sign):
        to = ring_index(lax.rem(pos + sign + n, n), n)
        at = gath.at[sending_slot, core * halves + q]
        return pltpu.make_async_remote_copy(
            src_ref=at, dst_ref=at, send_sem=ring_send.at[k, q], recv_sem=ring_recv.at[k, q],
            device_id=(f, to), device_id_type=MESH)

    def pair_copy(k, q, whose):
        at = gath.at[slot_of(k), whose * halves + q]
        return pltpu.make_async_remote_copy(
            src_ref=at, dst_ref=at, send_sem=pair_send.at[k, q], recv_sem=pair_recv.at[k, q],
            device_id=(f + 1 - 2 * core, me), device_id_type=MESH)

    def start_own():
        for q in range(halves):
            ring_copy(1, q, pos, 1).start()
            ring_copy(2, q, pos, -1).start()

    for c in own:
        c.wait()
    pl.semaphore_wait(barrier, len(near))
    start_own()
    for c in range(rows // EDGE):
        q = c % UNITS
        pltpu.matmul_push_rhs(m_tile(pos, c), 0, q, transpose=True)
        pltpu.matmul_acc_lhs(uaccs[0][q], pick[0], load_staged_rhs=0)
        pltpu.matmul_acc_lhs(uaccs[1][q], pick[1])
        left[0, c] = pltpu.matmul_pop(uaccs[0][q]).astype(jnp.bfloat16)
        left[1, c] = pltpu.matmul_pop(uaccs[1][q]).astype(jnp.bfloat16)

    def event(m):
        def plus():
            k, q = 2 * (m // halves) + 1, m % halves
            ring_copy(k, q, slot_of(k), 1).wait_recv()

            @pl.when((k + 2 < n - 1) | ((k + 2 == n - 1) & (q < split)))
            def _():
                ring_copy(k + 2, q, slot_of(k), 1).start()

            pair_copy(k, q, core).start()

        def minus():
            last = jnp.int32(m >= plan.whole) if isinstance(m, int) else (m >= plan.whole).astype(jnp.int32)
            k = (1 - last) * (2 * (m // halves) + 2) + last * (n - 1)
            q = (1 - last) * (m % halves) + last * (split + m - plan.whole)
            ring_copy(k, q, slot_of(k), -1).wait_recv()

            @pl.when((k + 2 < n - 1) | ((k == n - 2) & (q >= split)))
            def _():
                further = (k == n - 2).astype(jnp.int32)
                ring_copy((1 - further) * (k + 2) + further * (n - 1), q, slot_of(k), -1).start()

            pair_copy(k, q, core).start()

        pl.when(m < plan.plus)(plus)
        pl.when(m < plan.minus)(minus)

    def await_pair(k):
        for q in range(halves):
            pair_copy(k, q, 1 - core).wait_recv()

    def await_for(v):
        if per_block == 1:
            for q in range(UNITS):
                @pl.when((v >= 0) & (UNITS * v + q > 0))
                def _(q=q):
                    await_pair(UNITS * v + q)
        else:
            @pl.when((v > 0) & ((UNITS * v) % per_block == 0))
            def _():
                await_pair((UNITS * v) // per_block)

    def fence(t, j, final):
        slot = lax.rem(t, BUFFERS)
        if j < jobs - 1:
            wait_w(slot, j + 1)
        elif not final:
            wait_w(lax.rem(t + 1, BUFFERS), 0)

        if not final:
            @pl.when(t + BUFFERS < steps)
            def _():
                start_w(t + BUFFERS, slot, j)

        if j == jobs - 1 and not final:
            d = t - plan.first
            e = (d * plan.den + plan.num - 1) // plan.num
            due = (d >= 0) & ((e * plan.num) // plan.den == d) & (e < plan.rounds)

            def act(i, carry):
                event(e * plan.group + i)
                return carry

            lax.fori_loop(0, plan.group * due.astype(jnp.int32), act, 0)
            await_for(t + 1 - lag)

    def push_w(slot, j, part, c):
        for q in range(UNITS):
            pltpu.matmul_push_rhs(
                wbuf[slot, j, part, pl.ds(c * EDGE, EDGE), pl.ds(q * EDGE, EDGE)], 0, q)

    def push_v(v):
        for q in range(UNITS):
            i = UNITS * v + q
            pltpu.matmul_push_rhs(m_tile(slot_of(i // per_block), i % per_block), 0, q)

    def finish(t, j):
        for q in range(UNITS):
            value = weights[j] * pltpu.matmul_pop(uaccs[j % 3][q])
            if j > 0:
                value = uacc[q] + value
            if j < jobs - 1:
                uacc[q] = value
            else:
                high = value.astype(jnp.bfloat16)
                ubuf[t + 1, q, 0] = high
                ubuf[t + 1, q, 1] = (value - high.astype(jnp.float32)).astype(jnp.bfloat16)

    def v_part(v, part):
        for q in range(UNITS):
            pltpu.matmul_acc_lhs(vacc[q], ubuf[v + 1, q, part], load_staged_rhs=None if part else 0)

    def step(t, with_v, final=False):
        slot = lax.rem(t, BUFFERS)
        following = lax.rem(t + 1, BUFFERS)
        v = t - lag
        left_over = list(range(steps - 1 - lag, steps - 2))
        share = -(-len(left_over) // (jobs - 1))
        for j in range(jobs):
            for i, (part, c) in enumerate(chunks):
                end = i == len(chunks) - 1
                if end and not final and (j < jobs - 1 or not with_v):
                    fence(t, j, final)
                lhs = left[part, c]
                for q in range(UNITS):
                    pltpu.matmul_acc_lhs(uaccs[j % 3][q], lhs, load_staged_rhs=0)
                if not end:
                    push_w(slot, j, *chunks[i + 1])
                elif j < jobs - 1:
                    if final:
                        for extra in left_over[j * share:(j + 1) * share]:
                            push_v(extra)
                            v_part(extra, 0)
                            v_part(extra, 1)
                        fence(t, j, final)
                    push_w(slot, j + 1, *chunks[0])
                elif final:
                    push_v(steps - 2)
                elif with_v:
                    push_v(v)
                else:
                    push_w(following, 0, *chunks[0])
                if i == min(POP_AT, len(chunks) - 1):
                    if j == 0:
                        finish(t - 1, jobs - 1)
                    else:
                        finish(t, j - 1)
        if final:
            v_part(steps - 2, 0)
            v_part(steps - 2, 1)
        elif with_v:
            fence(t, jobs - 1, final)
            v_part(v, 0)
            push_w(following, 0, *chunks[0])
            v_part(v, 1)

    wait_w(0, 0)
    push_w(0, 0, *chunks[0])

    def early(t, carry):
        step(t, False)
        return carry

    def late(t, carry):
        step(t, True)
        return carry

    lax.fori_loop(0, lag, early, 0)
    lax.fori_loop(lag, steps - 1, late, 0)
    for v in range(steps - lag, steps):
        await_for(jnp.int32(v))
    pl.semaphore_signal(plane_sem, inc=1, device_id=twin, device_id_type=MESH)
    step(jnp.int32(steps - 1), True, final=True)
    finish(steps - 1, jobs - 1)
    push_v(steps - 1)
    v_part(steps - 1, 0)
    v_part(steps - 1, 1)

    total = pltpu.matmul_pop(vacc[0]) + pltpu.matmul_pop(vacc[1])
    p = total[:bands]
    r = total[bands:]
    real = p[:, :bands] - r[:, bands:]
    imag = p[:, bands:] + r[:, :bands]
    share = out_ref.shape[0]
    for d in range(devices):
        stage[d, :, pl.ds(0, bands)] = real[d * share:(d + 1) * share]
        stage[d, :, pl.ds(bands, bands)] = imag[d * share:(d + 1) * share]

    def give(r, carry):
        other = lax.rem(mine + r, devices)
        pltpu.make_async_remote_copy(
            src_ref=stage.at[other], dst_ref=inbox.at[r - 1], send_sem=out_send, recv_sem=out_recv,
            device_id=(other // n, other % n), device_id_type=MESH).start()
        return carry

    pl.semaphore_wait(plane_sem, 1)
    lax.fori_loop(1, devices, give, 0)
    for q in range(halves):
        for k in range(1, n):
            forward = k % 2 == 1 if k < n - 1 else q < split
            if k <= 2:
                source = pos
            elif k < n - 1:
                source = slot_of(k - 2)
            else:
                source = slot_of(n - 3 if forward else n - 2)
            ring_copy(k, q, source, 1 if forward else -1).wait_send()
            pair_copy(k, q, core).wait_send()
    pltpu.make_async_copy(inbox, inbox, out_recv).wait()
    out_ref[...] = stage[mine] + jnp.sum(inbox[...], axis=0)
    pltpu.make_async_copy(inbox, inbox, out_send).wait()


def on_device(n, nf, w_imag, w_real, pair_elements, quad_weight, residue_freq, owner_bands):
    fi, rows, width = w_imag.shape
    fr = w_real.shape[0]
    bands = owner_bands.shape[0]
    jobs = fi + fr
    plan = Plan(n, nf, rows, width // 2, jobs)
    devices = n * nf
    share = bands // devices
    dma = pltpu.SemaphoreType.DMA
    anyspace = pl.BlockSpec(memory_space=pl.ANY)
    vmem = pl.BlockSpec(memory_space=pltpu.VMEM)
    flops = 2 * jobs * rows * width * 2 * bands
    halves = plan.halves
    return pl.pallas_call(
        functools.partial(self_energy_kernel, plan),
        out_shape=jax.ShapeDtypeStruct((share, 2 * bands), jnp.float32),
        in_specs=[anyspace] * 6,
        out_specs=vmem,
        scratch_shapes=[
            pltpu.VMEM((BUFFERS, jobs, 2, rows, plan.tile), jnp.bfloat16),
            pltpu.VMEM((n, 2 * halves, plan.piece_rows, 2 * bands), jnp.bfloat16),
            pltpu.VMEM((2, rows // EDGE, 2 * bands, EDGE), jnp.bfloat16),
            pltpu.VMEM((jobs, 2 * bands, EDGE), jnp.float32),
            pltpu.VMEM((UNITS, 2 * bands, EDGE), jnp.float32),
            pltpu.VMEM((plan.steps + 1, UNITS, 2, 2 * bands, EDGE), jnp.bfloat16),
            pltpu.VMEM((fi, bands), jnp.float32),
            pltpu.VMEM((1, bands), jnp.int32),
            pltpu.VMEM((1, bands), jnp.int32),
            pltpu.VMEM((devices, share, 2 * bands), jnp.float32),
            pltpu.VMEM((devices - 1, share, 2 * bands), jnp.float32),
            dma((BUFFERS, jobs)),
            dma((2 * halves,)),
            dma((3,)),
            dma((n, halves)),
            dma((n, halves)),
            dma((n, halves)),
            dma((n, halves)),
            dma,
            dma,
            pltpu.SemaphoreType.REGULAR,
        ],
        compiler_params=pltpu.CompilerParams(
            collective_id=0, has_side_effects=True, vmem_limit_bytes=44 * 1024 * 1024),
        cost_estimate=pl.CostEstimate(
            flops=flops, bytes_accessed=jobs * rows * width * 2, transcendentals=0),
    )(*[pltpu.with_memory_space_constraint(x, pltpu.HBM) for x in (
        w_imag, w_real, pair_elements, quad_weight,
        residue_freq.reshape(1, bands), owner_bands.reshape(1, bands))])


def solution(mesh):
    placed = (
        P("freq", "gblk", None),
        P("freq", "gblk", None),
        P("gblk", None),
        P("freq", None),
        P(),
        P(),
    )
    body = functools.partial(on_device, mesh.shape["gblk"], mesh.shape["freq"])
    return jax.shard_map(
        body, mesh=mesh, in_specs=placed, out_specs=P(("freq", "gblk"), None), check_vma=False
    )
```

```python
import functools

import jax
import jax.numpy as jnp
from jax import lax
from jax.experimental import pallas as pl
from jax.experimental.pallas import tpu as pltpu
from jax.sharding import PartitionSpec as P

MESH = pl.DeviceIdType.MESH
EDGE = 256
UNITS = 2
BUFFERS = 4
POP_AT = 2
FIRST = 2


def ring_position(index, n):
    z = index // 2
    return z + (index % 2) * (n - 1 - 2 * z)


def ring_index(position, n):
    low = (position < n // 2).astype(jnp.int32)
    return low * (2 * position) + (1 - low) * (2 * (n - 1 - position) + 1)


class Plan:
    def __init__(self, n, nf, rows, g_count, jobs):
        assert n % 2 == 0 and n > 2 and nf == 4 and rows % EDGE == 0 and g_count % (UNITS * EDGE) == 0
        self.n, self.nf, self.rows, self.jobs = n, nf, rows, jobs
        self.devices = n * nf
        self.tile = UNITS * EDGE
        self.steps = g_count // self.tile
        self.per_block = rows // EDGE
        assert self.per_block == 1 or self.per_block % UNITS == 0
        self.halves = 2 if rows >= 1024 else 1
        self.piece_rows = rows // (2 * self.halves)
        self.pieces = EDGE // self.piece_rows
        self.split = (self.halves + 1) // 2
        whole = (n // 2 - 1) * self.halves
        self.plus = whole + self.split
        self.minus = whole + self.halves - self.split
        self.whole = whole
        self.events = max(self.plus, self.minus)
        self.group = -(-self.events // 7)
        self.rounds = -(-self.events // self.group)
        self.num, self.den, self.first = 3, 2, FIRST * self.steps // 16
        self.at = [self.first + ((m // self.group) * self.num) // self.den for m in range(self.events)]
        assert self.at[-1] <= self.steps - 3
        lag = 2
        for k in range(1, n):
            need = (k * self.per_block) // UNITS
            last = max(self.at[m] for m in range(self.events) if k in self.blocks_of(m))
            lag = max(lag, last + 2 - need)
        self.lag = min(lag, self.steps - 2)

    def blocks_of(self, m):
        found = []
        if m < self.plus:
            found.append(2 * (m // self.halves) + 1)
        if m < self.minus:
            found.append(min(2 * (m // self.halves) + 2, self.n - 1))
        return found


def self_energy_kernel(
    plan,
    wi_hbm, wr_hbm, m_hbm, quad_hbm, residue_hbm, owner_hbm, out_ref,
    wbuf, gath, left, weights, uacc, ubuf, quad_ref, residue_ref, owner_ref, stage, inbox,
    w_sem, own_sem, small_sem, ring_send, ring_recv, pair_send, pair_recv, out_send, out_recv, plane_sem,
):
    def body(*accs):
        run(
            plan, accs[:UNITS], (accs[UNITS:2 * UNITS], accs[2 * UNITS:3 * UNITS], accs[3 * UNITS:]),
            wi_hbm, wr_hbm, m_hbm, quad_hbm, residue_hbm, owner_hbm, out_ref,
            wbuf, gath, left, weights, uacc, ubuf, quad_ref, residue_ref, owner_ref, stage, inbox,
            w_sem, own_sem, small_sem, ring_send, ring_recv, pair_send, pair_recv, out_send, out_recv, plane_sem)

    shape = (EDGE, EDGE)
    pl.run_scoped(body, *[pltpu.ACC(i % UNITS)(shape, jnp.float32) for i in range(4 * UNITS)])


def run(
    plan, vacc, uaccs,
    wi_hbm, wr_hbm, m_hbm, quad_hbm, residue_hbm, owner_hbm, out_ref,
    wbuf, gath, left, weights, uacc, ubuf, quad_ref, residue_ref, owner_ref, stage, inbox,
    w_sem, own_sem, small_sem, ring_send, ring_recv, pair_send, pair_recv, out_send, out_recv, plane_sem,
):
    n, nf, rows, jobs = plan.n, plan.nf, plan.rows, plan.jobs
    halves, piece_rows, steps, lag = plan.halves, plan.piece_rows, plan.steps, plan.lag
    per_block, devices, split = plan.per_block, plan.devices, plan.split
    f = lax.axis_index("freq")
    me = lax.axis_index("gblk")
    pos = ring_position(me, n)
    core = f % 2
    fi = wi_hbm.shape[0]
    fr = wr_hbm.shape[0]
    g_count = wi_hbm.shape[2] // 2
    bands = owner_ref.shape[1]
    mine = f * n + me
    chunks = [(part, c) for part in range(2) for c in range(rows // EDGE)]

    def slot_of(k):
        d = (k + 1) // 2
        sign = 2 * (k % 2) - 1
        return lax.rem(pos - sign * d + 2 * n, n)

    def w_source(j, part, col, width):
        cols = pl.ds(pl.multiple_of(col + part * g_count, EDGE), width)
        return wi_hbm.at[j, :, cols] if j < fi else wr_hbm.at[j - fi, :, cols]

    def start_w(t, slot, j):
        for part in range(2):
            if per_block == 1:
                for q in range(UNITS):
                    col = ring_index(slot_of(UNITS * t + q), n) * rows
                    pltpu.make_async_copy(
                        w_source(j, part, col, EDGE),
                        wbuf.at[slot, j, part, :, pl.ds(q * EDGE, EDGE)], w_sem.at[slot, j]).start(priority=1)
            else:
                trips = per_block // UNITS
                col = ring_index(slot_of(t // trips), n) * rows + (t % trips) * plan.tile
                pltpu.make_async_copy(
                    w_source(j, part, col, plan.tile), wbuf.at[slot, j, part], w_sem.at[slot, j]).start(priority=1)

    def wait_w(slot, j):
        pltpu.make_async_copy(wbuf.at[slot, j], wbuf.at[slot, j], w_sem.at[slot, j]).wait()

    small = [
        pltpu.make_async_copy(owner_hbm, owner_ref, small_sem.at[0]),
        pltpu.make_async_copy(quad_hbm, quad_ref, small_sem.at[1]),
        pltpu.make_async_copy(residue_hbm, residue_ref, small_sem.at[2]),
    ]
    own = [pltpu.make_async_copy(
        m_hbm.at[pl.ds(i * piece_rows, piece_rows)], gath.at[pos, i], own_sem.at[i])
        for i in range(2 * halves)]
    for c in small + own:
        c.start()
    for t in range(min(BUFFERS, steps)):
        for j in range(jobs):
            start_w(t, t, j)

    barrier = pltpu.get_barrier_semaphore()

    pair = (f + 1 - 2 * core, me)
    twin = (lax.rem(f + 2, nf), me)
    near = [(f, ring_index(lax.rem(pos + 1, n), n)), (f, ring_index(lax.rem(pos + n - 1, n), n)), pair, twin]
    for other in near:
        pl.semaphore_signal(barrier, inc=1, device_id=other, device_id_type=MESH)

    for acc in list(vacc) + [a for pair in uaccs for a in pair]:
        pltpu.matmul_pop(acc)
    uacc[...] = jnp.zeros_like(uacc)

    for c in small:
        c.wait()
    onehot_t = (lax.broadcasted_iota(jnp.int32, (bands, bands), 0) == owner_ref[...]).astype(jnp.float32)
    onehot = jnp.transpose(onehot_t)
    for j in range(jobs):
        if j < fi:
            row = quad_ref[pl.ds(j, 1), :]
        else:
            row = (residue_ref[...] == f * fr + (j - fi)).astype(jnp.float32)
        column = jnp.broadcast_to(jnp.sum(onehot * row, axis=1, keepdims=True), (bands, EDGE))
        weights[j, pl.ds(0, bands), :] = column
        weights[j, pl.ds(bands, bands), :] = column
    nothing = jnp.zeros_like(onehot)
    pick = (
        jnp.concatenate([jnp.concatenate([onehot, nothing], axis=1),
                         jnp.concatenate([nothing, 0.0 - onehot], axis=1)], axis=0).astype(jnp.bfloat16),
        jnp.concatenate([jnp.concatenate([nothing, onehot], axis=1),
                         jnp.concatenate([onehot, nothing], axis=1)], axis=0).astype(jnp.bfloat16),
    )

    def m_tile(slot, sub):
        return gath[slot, pl.ds(sub * plan.pieces, plan.pieces)].reshape(EDGE, 2 * bands)

    def ring_copy(k, q, sending_slot, sign):
        to = ring_index(lax.rem(pos + sign + n, n), n)
        at = gath.at[sending_slot, core * halves + q]
        return pltpu.make_async_remote_copy(
            src_ref=at, dst_ref=at, send_sem=ring_send.at[k, q], recv_sem=ring_recv.at[k, q],
            device_id=(f, to), device_id_type=MESH)

    def pair_copy(k, q, whose):
        at = gath.at[slot_of(k), whose * halves + q]
        return pltpu.make_async_remote_copy(
            src_ref=at, dst_ref=at, send_sem=pair_send.at[k, q], recv_sem=pair_recv.at[k, q],
            device_id=(f + 1 - 2 * core, me), device_id_type=MESH)

    def start_own():
        for q in range(halves):
            ring_copy(1, q, pos, 1).start()
            ring_copy(2, q, pos, -1).start()

    for c in own:
        c.wait()
    pl.semaphore_wait(barrier, len(near))
    start_own()
    for c in range(rows // EDGE):
        q = c % UNITS
        pltpu.matmul_push_rhs(m_tile(pos, c), 0, q, transpose=True)
        pltpu.matmul_acc_lhs(uaccs[0][q], pick[0], load_staged_rhs=0)
        pltpu.matmul_acc_lhs(uaccs[1][q], pick[1])
        left[0, c] = pltpu.matmul_pop(uaccs[0][q]).astype(jnp.bfloat16)
        left[1, c] = pltpu.matmul_pop(uaccs[1][q]).astype(jnp.bfloat16)

    def event(m):
        def plus():
            k, q = 2 * (m // halves) + 1, m % halves
            ring_copy(k, q, slot_of(k), 1).wait_recv()

            @pl.when((k + 2 < n - 1) | ((k + 2 == n - 1) & (q < split)))
            def _():
                ring_copy(k + 2, q, slot_of(k), 1).start()

            pair_copy(k, q, core).start()

        def minus():
            last = jnp.int32(m >= plan.whole) if isinstance(m, int) else (m >= plan.whole).astype(jnp.int32)
            k = (1 - last) * (2 * (m // halves) + 2) + last * (n - 1)
            q = (1 - last) * (m % halves) + last * (split + m - plan.whole)
            ring_copy(k, q, slot_of(k), -1).wait_recv()

            @pl.when((k + 2 < n - 1) | ((k == n - 2) & (q >= split)))
            def _():
                further = (k == n - 2).astype(jnp.int32)
                ring_copy((1 - further) * (k + 2) + further * (n - 1), q, slot_of(k), -1).start()

            pair_copy(k, q, core).start()

        pl.when(m < plan.plus)(plus)
        pl.when(m < plan.minus)(minus)

    def await_pair(k):
        for q in range(halves):
            pair_copy(k, q, 1 - core).wait_recv()

    def await_for(v):
        if per_block == 1:
            for q in range(UNITS):
                @pl.when((v >= 0) & (UNITS * v + q > 0))
                def _(q=q):
                    await_pair(UNITS * v + q)
        else:
            @pl.when((v > 0) & ((UNITS * v) % per_block == 0))
            def _():
                await_pair((UNITS * v) // per_block)

    def fence(t, j, final):
        slot = lax.rem(t, BUFFERS)
        if j < jobs - 1:
            wait_w(slot, j + 1)
        elif not final:
            wait_w(lax.rem(t + 1, BUFFERS), 0)

        if not final:
            @pl.when(t + BUFFERS < steps)
            def _():
                start_w(t + BUFFERS, slot, j)

        if j == jobs - 1 and not final:
            d = t - plan.first
            e = (d * plan.den + plan.num - 1) // plan.num
            due = (d >= 0) & ((e * plan.num) // plan.den == d) & (e < plan.rounds)

            def act(i, carry):
                event(e * plan.group + i)
                return carry

            lax.fori_loop(0, plan.group * due.astype(jnp.int32), act, 0)
            await_for(t + 1 - lag)

    def push_w(slot, j, part, c):
        for q in range(UNITS):
            pltpu.matmul_push_rhs(
                wbuf[slot, j, part, pl.ds(c * EDGE, EDGE), pl.ds(q * EDGE, EDGE)], 0, q)

    def push_v(v):
        for q in range(UNITS):
            i = UNITS * v + q
            pltpu.matmul_push_rhs(m_tile(slot_of(i // per_block), i % per_block), 0, q)

    def finish(t, j):
        for q in range(UNITS):
            value = weights[j] * pltpu.matmul_pop(uaccs[j % 3][q])
            if j > 0:
                value = uacc[q] + value
            if j < jobs - 1:
                uacc[q] = value
            else:
                high = value.astype(jnp.bfloat16)
                ubuf[t + 1, q, 0] = high
                ubuf[t + 1, q, 1] = (value - high.astype(jnp.float32)).astype(jnp.bfloat16)

    def v_part(v, part):
        for q in range(UNITS):
            pltpu.matmul_acc_lhs(vacc[q], ubuf[v + 1, q, part], load_staged_rhs=None if part else 0)

    def step(t, with_v, final=False):
        slot = lax.rem(t, BUFFERS)
        following = lax.rem(t + 1, BUFFERS)
        v = t - lag
        left_over = list(range(steps - 1 - lag, steps - 2))
        share = -(-len(left_over) // (jobs - 1))
        for j in range(jobs):
            for i, (part, c) in enumerate(chunks):
                end = i == len(chunks) - 1
                if end and not final and (j < jobs - 1 or not with_v):
                    fence(t, j, final)
                lhs = left[part, c]
                for q in range(UNITS):
                    pltpu.matmul_acc_lhs(uaccs[j % 3][q], lhs, load_staged_rhs=0)
                if not end:
                    push_w(slot, j, *chunks[i + 1])
                elif j < jobs - 1:
                    if final:
                        for extra in left_over[j * share:(j + 1) * share]:
                            push_v(extra)
                            v_part(extra, 0)
                            v_part(extra, 1)
                        fence(t, j, final)
                    push_w(slot, j + 1, *chunks[0])
                elif final:
                    push_v(steps - 2)
                elif with_v:
                    push_v(v)
                else:
                    push_w(following, 0, *chunks[0])
                if i == min(POP_AT, len(chunks) - 1):
                    if j == 0:
                        finish(t - 1, jobs - 1)
                    else:
                        finish(t, j - 1)
        if final:
            v_part(steps - 2, 0)
            v_part(steps - 2, 1)
        elif with_v:
            fence(t, jobs - 1, final)
            v_part(v, 0)
            push_w(following, 0, *chunks[0])
            v_part(v, 1)

    wait_w(0, 0)
    push_w(0, 0, *chunks[0])

    def early(t, carry):
        step(t, False)
        return carry

    def late(t, carry):
        step(t, True)
        return carry

    lax.fori_loop(0, lag, early, 0)
    lax.fori_loop(lag, steps - 1, late, 0)
    for v in range(steps - lag, steps):
        await_for(jnp.int32(v))
    pl.semaphore_signal(plane_sem, inc=1, device_id=twin, device_id_type=MESH)
    step(jnp.int32(steps - 1), True, final=True)
    finish(steps - 1, jobs - 1)
    push_v(steps - 1)
    v_part(steps - 1, 0)
    v_part(steps - 1, 1)

    total = pltpu.matmul_pop(vacc[0]) + pltpu.matmul_pop(vacc[1])
    p = total[:bands]
    r = total[bands:]
    real = p[:, :bands] - r[:, bands:]
    imag = p[:, bands:] + r[:, :bands]
    share = out_ref.shape[0]
    for d in range(devices):
        stage[d, :, pl.ds(0, bands)] = real[d * share:(d + 1) * share]
        stage[d, :, pl.ds(bands, bands)] = imag[d * share:(d + 1) * share]

    deep = n // 2
    order = [(df, dz, dy)
             for dz in sorted(range(deep), key=lambda dz: -min(dz, deep - dz))
             for df in (2, 1, 3, 0) for dy in (1, 0)]
    order.remove((0, 0, 0))
    pl.semaphore_wait(plane_sem, 1)
    for i, (df, dz, dy) in enumerate(order):
        other_f = lax.rem(f + df, nf)
        other_g = 2 * lax.rem(me // 2 + dz, deep) + lax.rem(me % 2 + dy, 2)
        pltpu.make_async_remote_copy(
            src_ref=stage.at[other_f * n + other_g], dst_ref=inbox.at[i], send_sem=out_send, recv_sem=out_recv,
            device_id=(other_f, other_g), device_id_type=MESH).start()
    for q in range(halves):
        for k in range(1, n):
            forward = k % 2 == 1 if k < n - 1 else q < split
            if k <= 2:
                source = pos
            elif k < n - 1:
                source = slot_of(k - 2)
            else:
                source = slot_of(n - 3 if forward else n - 2)
            ring_copy(k, q, source, 1 if forward else -1).wait_send()
            pair_copy(k, q, core).wait_send()
    pltpu.make_async_copy(inbox, inbox, out_recv).wait()
    out_ref[...] = stage[mine] + jnp.sum(inbox[...], axis=0)
    pltpu.make_async_copy(inbox, inbox, out_send).wait()


def on_device(n, nf, w_imag, w_real, pair_elements, quad_weight, residue_freq, owner_bands):
    fi, rows, width = w_imag.shape
    fr = w_real.shape[0]
    bands = owner_bands.shape[0]
    jobs = fi + fr
    plan = Plan(n, nf, rows, width // 2, jobs)
    devices = n * nf
    share = bands // devices
    dma = pltpu.SemaphoreType.DMA
    anyspace = pl.BlockSpec(memory_space=pl.ANY)
    vmem = pl.BlockSpec(memory_space=pltpu.VMEM)
    flops = 2 * jobs * rows * width * 2 * bands
    halves = plan.halves
    return pl.pallas_call(
        functools.partial(self_energy_kernel, plan),
        out_shape=jax.ShapeDtypeStruct((share, 2 * bands), jnp.float32),
        in_specs=[anyspace] * 6,
        out_specs=vmem,
        scratch_shapes=[
            pltpu.VMEM((BUFFERS, jobs, 2, rows, plan.tile), jnp.bfloat16),
            pltpu.VMEM((n, 2 * halves, plan.piece_rows, 2 * bands), jnp.bfloat16),
            pltpu.VMEM((2, rows // EDGE, 2 * bands, EDGE), jnp.bfloat16),
            pltpu.VMEM((jobs, 2 * bands, EDGE), jnp.float32),
            pltpu.VMEM((UNITS, 2 * bands, EDGE), jnp.float32),
            pltpu.VMEM((plan.steps + 1, UNITS, 2, 2 * bands, EDGE), jnp.bfloat16),
            pltpu.VMEM((fi, bands), jnp.float32),
            pltpu.VMEM((1, bands), jnp.int32),
            pltpu.VMEM((1, bands), jnp.int32),
            pltpu.VMEM((devices, share, 2 * bands), jnp.float32),
            pltpu.VMEM((devices - 1, share, 2 * bands), jnp.float32),
            dma((BUFFERS, jobs)),
            dma((2 * halves,)),
            dma((3,)),
            dma((n, halves)),
            dma((n, halves)),
            dma((n, halves)),
            dma((n, halves)),
            dma,
            dma,
            pltpu.SemaphoreType.REGULAR,
        ],
        compiler_params=pltpu.CompilerParams(
            collective_id=0, has_side_effects=True, vmem_limit_bytes=44 * 1024 * 1024),
        cost_estimate=pl.CostEstimate(
            flops=flops, bytes_accessed=jobs * rows * width * 2, transcendentals=0),
    )(*[pltpu.with_memory_space_constraint(x, pltpu.HBM) for x in (
        w_imag, w_real, pair_elements, quad_weight,
        residue_freq.reshape(1, bands), owner_bands.reshape(1, bands))])


def solution(mesh):
    placed = (
        P("freq", "gblk", None),
        P("freq", "gblk", None),
        P("gblk", None),
        P("freq", None),
        P(),
        P(),
    )
    body = functools.partial(on_device, mesh.shape["gblk"], mesh.shape["freq"])
    return jax.shard_map(
        body, mesh=mesh, in_specs=placed, out_specs=P(("freq", "gblk"), None), check_vma=False
    )
```
